128 devices in a mesh: row: 8 (over x, y_hi), col: 16 (over z, y_lo, core).
Axes of the slice: x: 4, y: 4 (y_hi: 2, y_lo: 2; y = y_hi * 2 + y_lo), z: 4, core: 2. Of those that a mesh axis runs over, the one named last changes fastest.
Arguments:
- old_residual: float32 [8192, 16384], P(('row', 'col')), may hold values from -6 to 6
- group_map: int32 [128, 8], replicated, may hold values from 0 to 1023, as said below
- q_factor: float32 [16384, 32], P('col', 'row'), may hold values from -0.046875 to 0.046875
Outputs:
- relaid: float32 [8192, 16384], P('row', 'col')
- projection: float32 [32, 8192], P(None, ('row', 'col'))
- row_norms: float32 [8192], P(('row', 'col'))
The draws below stay inside these ranges and needn't reach their ends.
Inputs may be any that keep to these rules, and one draw needn't show every extreme that they name: `group_map`: all entries together are each group id 0 to 1023 once; row d (old device d) holds exactly one id of each range k * 128 to (k + 1) * 128 - 1, in any slot order.
All inputs are finite; a program needn't handle non-finite values.
Results may differ from the reference program's by a relative error of at most 0.00007.
Values sent between devices are 32-bit elements; how exact they have to be, the bound alone decides.
A program may use at most 64 MiB of HBM per device.

```python
import jax
import jax.numpy as jnp
from jax import lax

D = 16384
RANK = 32
CH = 8
ROWS = 8192
N_ROW = 8
DEVICES = 128


def draw_group_map(key, part):
    first_key = jax.random.fold_in(key, 11)
    second_key = jax.random.fold_in(key, 23)
    block_keys = jax.random.split(first_key, N_ROW)
    permuted = jax.vmap(lambda single: jax.random.permutation(single, DEVICES))(block_keys)
    group_ids = (permuted + jnp.arange(N_ROW, dtype=jnp.int32)[:, None] * DEVICES).T
    slot_keys = jax.random.split(second_key, DEVICES)
    slot_order = jax.vmap(lambda single: jax.random.permutation(single, N_ROW))(slot_keys)
    return jnp.take_along_axis(group_ids, slot_order, axis=1).astype(jnp.int32)


def shard_levels(key, shape, pieces, low, high):
    gain = 1.0
    for position, parts in pieces:
        steps = jax.random.uniform(jax.random.fold_in(jax.random.fold_in(key, 6), position), (parts,), jnp.float32, low / len(pieces), high / len(pieces))
        gain = gain * jnp.repeat(jnp.exp(steps), shape[position] // parts).reshape((-1,) + (1,) * (len(shape) - 1 - position))
    return gain


def normal_values(key, shape, deviation, bound, pieces=(), kind=jnp.bfloat16):
    array = deviation * jax.random.normal(key, shape, jnp.float32)
    if pieces:
        array = array * shard_levels(key, shape, pieces, -0.22, 0.18)
    return jnp.clip(array, -bound, bound).astype(kind)


def setup_inputs(seed: int = 0) -> dict:
    streams_of = jax.random.split(jax.random.key(seed), 4)
    return {
        "old_residual": normal_values(streams_of[0], (ROWS, D), 1.0, 6.0, ((0, 128),), jnp.float32),
        "group_map": draw_group_map(jax.random.fold_in(streams_of[3], 71), 0),
        "q_factor": normal_values(streams_of[2], (D, RANK), D ** -0.5, 0.046875, ((0, 16), (1, 8)), jnp.float32),
    }


epsilon = 1e-06

def reference(old_residual, group_map, q_factor):
    group_ids = group_map.reshape(-1).astype(jnp.int32)
    ordering = jnp.argsort(group_ids).astype(jnp.int32)
    groups = old_residual.reshape(DEVICES * N_ROW, CH, D)
    relaid = jnp.take(groups, ordering, axis=0).reshape(ROWS, D)
    product = jnp.dot(relaid, q_factor, precision=lax.Precision.HIGHEST, preferred_element_type=jnp.float32)
    row_norms = jnp.sqrt(lax.optimization_barrier(jnp.mean(relaid * relaid, axis=1)) + epsilon)
    return (relaid, product.T, row_norms)
```

```python
import functools

import jax
import jax.numpy as jnp
from jax import lax
from jax.experimental import pallas as pl
from jax.experimental.pallas import tpu as pltpu
from jax.sharding import PartitionSpec as P

epsilon = 1e-06
MESH = pl.DeviceIdType.MESH
ROWS, COLS = 8, 16
DEVS = ROWS * COLS
CHUNK = 8
CHUNKS = DEVS // CHUNK
STEP = 51


def place():
    row, col = lax.axis_index("row"), lax.axis_index("col")
    return row, col


def shifted(row, col, n, sign):
    o = lax.rem(STEP * (n + 1), DEVS)
    bit = lambda i: lax.rem(lax.div(o, 2**i), 2)
    dx = bit(0) + 2 * bit(3)
    dy = bit(1) + 2 * bit(4)
    dz = bit(2) + 2 * bit(5)
    dk = bit(6)
    x = lax.div(row, 2)
    y = lax.rem(row, 2) * 2 + lax.rem(lax.div(col, 2), 2)
    z = lax.div(col, 4)
    k = lax.rem(col, 2)
    x = lax.rem(x + 4 + sign * dx, 4)
    y = lax.rem(y + 4 + sign * dy, 4)
    z = lax.rem(z + 4 + sign * dz, 4)
    k = lax.rem(k + dk, 2)
    return x * 2 + lax.div(y, 2), z * 4 + lax.rem(y, 2) * 2 + k


def kernel(
    old, gmap_s, gmap_v, q_own, relaid, p_out, norm_out,
    stage, send, recv, q_all, w_rows, w, p_part, s_part, p_send, p_recv, inv_v, inv_s,
    in_sem, inv_sem, q_ssem, q_rsem, ssem, rsem, p_ssem, p_rsem,
):
    row, col = place()
    me = row * COLS + col
    for j in range(ROWS):
        pltpu.make_async_copy(old.at[j], stage.at[j], in_sem.at[j]).start()

    barrier = pltpu.get_barrier_semaphore()

    @pl.loop(1, DEVS)
    def _(i):
        peer = lax.rem(me + i, DEVS)
        pl.semaphore_signal(
            barrier, inc=1, device_id=(lax.div(peer, COLS), lax.rem(peer, COLS)), device_id_type=MESH
        )

    slots = []
    for k in range(ROWS):
        slot = jnp.int32(0)
        for j in range(ROWS):
            slot += jnp.where(lax.shift_right_arithmetic(gmap_s[j, me], 7) == k, j, 0)
        slots.append(lax.bitwise_and(slot, 7))
    for j in range(ROWS):
        pltpu.make_async_copy(old.at[j], stage.at[j], in_sem.at[j]).wait()
    for k in range(ROWS):
        for c in range(COLS):
            send[k * COLS + c] = stage[slots[k], :, c * 1024 : (c + 1) * 1024]
    pl.semaphore_wait(barrier, DEVS - 1)

    @pl.loop(1, ROWS)
    def _(r):
        pltpu.make_async_remote_copy(
            src_ref=q_own, dst_ref=q_all.at[row], send_sem=q_ssem, recv_sem=q_rsem,
            device_id=(lax.rem(row + r, ROWS), col), device_id_type=MESH,
        ).start()

    @pl.loop(0, DEVS - 1)
    def _(n):
        r, c = shifted(row, col, n, 1)
        pltpu.make_async_remote_copy(
            src_ref=send.at[r * COLS + c], dst_ref=recv.at[me], send_sem=ssem,
            recv_sem=rsem.at[lax.div(n, CHUNK)], device_id=(r, c), device_id_type=MESH,
        ).start()

    recv[me] = send[me]
    q_all[row] = q_own[...]

    ids = gmap_v[...]
    mine = lax.shift_right_arithmetic(ids, 7) == row
    where_to = jnp.sum(jnp.where(mine, lax.bitwise_and(ids, 127), 0), axis=0, keepdims=True)
    spread = jnp.transpose(jnp.broadcast_to(where_to, (DEVS, DEVS)))
    lanes = lax.broadcasted_iota(jnp.int32, (DEVS, DEVS), 1)
    sources = lax.broadcasted_iota(jnp.int32, (DEVS, DEVS), 0)
    inverse = jnp.sum(jnp.where(spread == lanes, sources, 0), axis=0, keepdims=True)
    inv_v[...] = jnp.broadcast_to(lax.bitwise_and(inverse, 127), (8, DEVS))
    pltpu.make_async_copy(inv_v, inv_s, inv_sem).start()

    q7 = q_all.at[pl.ds(0, ROWS - 1)]
    pltpu.make_async_remote_copy(
        src_ref=q7, dst_ref=q7, send_sem=q_ssem, recv_sem=q_rsem, device_id=(row, col), device_id_type=MESH
    ).wait()
    for r in range(ROWS):
        for i in range(4):
            w_rows[32 * i + 4 * r : 32 * i + 4 * r + 4, :] = q_all[r]
    w[...] = jnp.transpose(w_rows[...])

    def multiply(i):
        blocks, at = [], []
        for j in range(CHUNK):
            r, c = shifted(row, col, i * CHUNK + j, -1)
            at.append(r * COLS + c)
            blocks.append(recv[at[-1]])
        rows = jnp.concatenate(blocks, axis=0)
        part = jnp.dot(rows, w[...], precision=lax.Precision.HIGHEST, preferred_element_type=jnp.float32)
        squares = jnp.sum(rows * rows, axis=1, keepdims=True)
        for j in range(CHUNK):
            p_part[at[j]] = part[8 * j : 8 * j + 8]
            s_part[at[j]] = jnp.broadcast_to(squares[8 * j : 8 * j + 8], (8, 128))

    def arrived(i, count):
        v = recv.at[pl.ds(0, count)]
        pltpu.make_async_remote_copy(
            src_ref=v, dst_ref=v, send_sem=ssem, recv_sem=rsem.at[i], device_id=(row, col), device_id_type=MESH
        ).wait_recv()

    @pl.loop(0, CHUNKS - 1)
    def _(i):
        arrived(i, CHUNK)
        multiply(i)

    arrived(CHUNKS - 1, CHUNK - 1)
    multiply(CHUNKS - 1)

    pltpu.make_async_copy(inv_v, inv_s, inv_sem).wait()
    lane = lax.broadcasted_iota(jnp.int32, (8, 128), 1)

    @pl.loop(0, COLS)
    def _(c):
        for t in range(2):
            tile = p_part[inv_s[0, c * 8 + t * 4]]
            for i in range(1, 4):
                tile = jnp.where(lane < 32 * i, tile, p_part[inv_s[0, c * 8 + t * 4 + i]])
            p_send[c, t] = tile
        tile = s_part[inv_s[0, c * 8]]
        for i in range(1, 8):
            tile = jnp.where(lane < 16 * i, tile, s_part[inv_s[0, c * 8 + i]])
        p_send[c, 2] = tile

    @pl.loop(1, COLS)
    def _(i):
        c = lax.rem(col + i, COLS)
        pltpu.make_async_remote_copy(
            src_ref=p_send.at[c], dst_ref=p_recv.at[col], send_sem=p_ssem, recv_sem=p_rsem,
            device_id=(row, c), device_id_type=MESH,
        ).start()

    p_recv[col] = p_send[col]

    @pl.loop(0, DEVS, unroll=8)
    def _(p):
        relaid[p] = recv[inv_s[0, p]]

    p15 = p_recv.at[pl.ds(0, COLS - 1)]
    pltpu.make_async_remote_copy(
        src_ref=p15, dst_ref=p15, send_sem=p_ssem, recv_sem=p_rsem, device_id=(row, col), device_id_type=MESH
    ).wait()
    total = p_recv[0]
    for c in range(1, COLS):
        total = total + p_recv[c]
    rows = []
    for g in range(8):
        t, i = divmod(g, 4)
        values = total[t] if i == 0 else pltpu.roll(total[t], 128 - 32 * i, axis=1)
        norms = pltpu.roll(total[2], (128 + 32 - 16 * g) % 128, axis=1) if g != 2 else total[2]
        rows.append(jnp.where(lane < 32, values, norms))
    flat = jnp.concatenate(rows + rows, axis=0)
    turned = jnp.transpose(flat)
    p_out[...] = turned[0:32, 0:64]
    norm_out[...] = jnp.sqrt(turned[32:33, 0:64] / 16384.0 + epsilon)

    v = recv.at[pl.ds(0, DEVS - 1)]
    pltpu.make_async_remote_copy(
        src_ref=v, dst_ref=v, send_sem=ssem, recv_sem=rsem.at[0], device_id=(row, col), device_id_type=MESH
    ).wait_send()


def on_device(old_residual, group_map, q_factor):
    f32 = jnp.float32
    ids = group_map.T
    vmem = pl.BlockSpec(memory_space=pltpu.VMEM)
    dma = pltpu.SemaphoreType.DMA
    relaid, projection, norms = pl.pallas_call(
        kernel,
        out_shape=(
            jax.ShapeDtypeStruct((DEVS, 8, 1024), f32),
            jax.ShapeDtypeStruct((32, 64), f32),
            jax.ShapeDtypeStruct((1, 64), f32),
        ),
        in_specs=[
            pl.BlockSpec(memory_space=pl.ANY),
            pl.BlockSpec(memory_space=pltpu.SMEM),
            vmem,
            vmem,
        ],
        out_specs=(vmem, vmem, vmem),
        scratch_shapes=[
            pltpu.VMEM((ROWS, 8, 16384), f32),
            pltpu.VMEM((DEVS, 8, 1024), f32),
            pltpu.VMEM((DEVS, 8, 1024), f32),
            pltpu.VMEM((ROWS, 4, 1024), f32),
            pltpu.VMEM((128, 1024), f32),
            pltpu.VMEM((1024, 128), f32),
            pltpu.VMEM((DEVS, 8, 128), f32),
            pltpu.VMEM((DEVS, 8, 128), f32),
            pltpu.VMEM((COLS, 3, 8, 128), f32),
            pltpu.VMEM((COLS, 3, 8, 128), f32),
            pltpu.VMEM((8, 128), jnp.int32),
            pltpu.SMEM((8, 128), jnp.int32),
            dma((ROWS,)),
            dma,
            dma,
            dma,
            dma,
            dma((CHUNKS,)),
            dma,
            dma,
        ],
        compiler_params=pltpu.CompilerParams(
            collective_id=0, has_side_effects=True, vmem_limit_bytes=48 << 20
        ),
    )(old_residual.reshape(ROWS, 8, 16384), ids, ids, q_factor.T)
    return relaid.reshape(1024, 1024), projection, norms.reshape(64)


def solution(mesh):
    return jax.shard_map(
        on_device,
        mesh=mesh,
        in_specs=(P(("row", "col"), None), P(), P("col", "row")),
        out_specs=(P("row", "col"), P(None, ("row", "col")), P(("row", "col"))),
        check_vma=False,
    )
```

```python
import jax
import jax.numpy as jnp
from jax import lax
from jax.experimental import pallas as pl
from jax.experimental.pallas import tpu as pltpu
from jax.sharding import PartitionSpec as P

epsilon = 1e-06
MESH = pl.DeviceIdType.MESH
ROWS, COLS = 8, 16
DEVS = ROWS * COLS
CHUNK = 8
CHUNKS = DEVS // CHUNK


def order():
    offsets = []
    for n in range(DEVS):
        c = 1 + MULT_C * n % 15 if n < DEVS - ROWS else 0
        s = MULT_S * (n + 1) % ROWS
        v = {name: c >> i & 1 for i, name in enumerate(BITS_C)} | {name: s >> i & 1 for i, name in enumerate(BITS_S)}
        offsets.append((v["x0"] + 2 * v["x1"], v["y0"] + 2 * v["y1"], v["z0"] + 2 * v["z1"], v["k"]))
    return offsets


MULT_C, MULT_S = 7, 3
BITS_C, BITS_S = ("z0", "z1", "y0", "k"), ("x0", "x1", "y1")
EARLY = 96
ORDER = order()
HOPS = (0, 1, 2, 1)


class Place:
    def __init__(self):
        row, col = lax.axis_index("row"), lax.axis_index("col")
        x, z, core = lax.div(row, 2), lax.div(col, 4), lax.rem(col, 2)
        y = lax.rem(row, 2) * 2 + lax.rem(lax.div(col, 2), 2)
        ys = [lax.rem(y + d, 4) for d in range(4)]
        self.row, self.col, self.me = row, col, row * COLS + col
        self.x_row = [2 * lax.rem(x + d, 4) for d in range(4)]
        self.y_row = [lax.div(v, 2) for v in ys]
        self.y_col = [2 * lax.rem(v, 2) for v in ys]
        self.z_col = [4 * lax.rem(z + d, 4) for d in range(4)]
        self.core = [core, 1 - core]

    def at(self, o):
        return self.x_row[o[0]] + self.y_row[o[1]], self.z_col[o[2]] + self.y_col[o[1]] + self.core[o[3]]

    def back(self, o):
        row, col = self.at((-o[0] % 4, -o[1] % 4, -o[2] % 4, o[3]))
        return row * COLS + col


def distance(o):
    return HOPS[o[0]] + HOPS[o[1]] + HOPS[o[2]] + 0.25 * o[3]


def exchange(
    old, ids, q_own, relaid, p_recv, s_recv,
    stage, send, recv, ids_s, ids_v, q_mine, q_all, w_rows, w, part, own_part, p_send, s_send,
    inv_v, inv_s, slot_s, from_s, here_s,
    in_sem, ids_sem, inv_sem, q_sem, q_ssem, q_rsem, ssem, rsem, o_ssem, o_rsem, p_ssem, p_rsem, s_ssem, s_rsem,
):
    here = Place()
    row, col, me = here.row, here.col, here.me

    def remote(src, dst, send_sem, recv_sem, to):
        return pltpu.make_async_remote_copy(
            src_ref=src, dst_ref=dst, send_sem=send_sem, recv_sem=recv_sem, device_id=to, device_id_type=MESH
        )

    ids_copy = pltpu.make_async_copy(ids, ids_s, ids_sem.at[0])
    ids_copy2 = pltpu.make_async_copy(ids, ids_v, ids_sem.at[1])
    q_copy = pltpu.make_async_copy(q_own, q_mine, q_sem)
    ids_copy.start()
    loads = []
    for j in range(ROWS):
        loads.append(pltpu.make_async_copy(old.at[j], stage.at[j], in_sem.at[j]))
        loads[-1].start()
    q_copy.start()
    ids_copy2.start()

    barrier = pltpu.get_barrier_semaphore()
    for o in sorted(ORDER[:-1], key=distance, reverse=True):
        pl.semaphore_signal(barrier, inc=1, device_id=here.at(o), device_id_type=MESH)

    ids_copy.wait()
    for k in range(ROWS):
        slot = jnp.int32(0)
        for j in range(ROWS):
            slot += jnp.where(lax.shift_right_arithmetic(ids_s[j, me], 7) == k, j, 0)
        slot_s[k] = lax.bitwise_and(slot, 7)

    for load in loads:
        load.wait()

    for n, o in enumerate(ORDER):
        r, c = here.at(o)
        send[n] = stage[slot_s[r], :, pl.ds(pl.multiple_of(c * 1024, 1024), 1024)]

    def send_blocks(first, last):
        for n in range(first, last):
            remote(send.at[n], recv.at[n], ssem, rsem.at[n // CHUNK], here.at(ORDER[n])).start()

    q_copy.wait()
    pl.semaphore_wait(barrier, DEVS - 1)
    for dx, a in [(2, 1), (1, 1), (3, 1), (2, 0), (0, 1), (1, 0), (3, 0)]:
        remote(q_mine, q_all.at[row], q_ssem, q_rsem, here.at((dx, 2 * a, 0, 0))).start()
    send_blocks(0, EARLY)

    q_all[row] = q_mine[...]
    recv[DEVS - 1] = send[DEVS - 1]

    ids_copy2.wait()
    held = ids_v[...]
    mine = lax.shift_right_arithmetic(held, 7) == row
    where_to = jnp.sum(jnp.where(mine, lax.bitwise_and(held, 127), 0), axis=0, keepdims=True)
    spread = jnp.transpose(jnp.broadcast_to(where_to, (DEVS, DEVS)))
    lanes = lax.broadcasted_iota(jnp.int32, (DEVS, DEVS), 1)
    sources = lax.broadcasted_iota(jnp.int32, (DEVS, DEVS), 0)
    inverse = jnp.sum(jnp.where(spread == lanes, sources, 0), axis=0, keepdims=True)
    inv_v[...] = jnp.broadcast_to(lax.bitwise_and(inverse, 127), (8, DEVS))
    inv_copy = pltpu.make_async_copy(inv_v, inv_s, inv_sem)
    inv_copy.start()
    for n, o in enumerate(ORDER):
        from_s[here.back(o)] = n

    remote(q_all.at[pl.ds(0, ROWS - 1)], q_all.at[pl.ds(0, ROWS - 1)], q_ssem, q_rsem, (row, col)).wait()
    for r in range(ROWS):
        for i in range(4):
            w_rows[32 * i + 4 * r : 32 * i + 4 * r + 4, :] = q_all[r]
    w_all = jnp.transpose(w_rows[...])
    w_high = w_all.astype(jnp.bfloat16)
    w[:, 0:128] = w_high
    w[:, 128:256] = (w_all - w_high.astype(jnp.float32)).astype(jnp.bfloat16)

    def multiply(rows, to):
        high = rows.astype(jnp.bfloat16)
        low = (rows - high.astype(jnp.float32)).astype(jnp.bfloat16)
        first = jnp.dot(high, w[...], preferred_element_type=jnp.float32)
        second = jnp.dot(low, w[:, 0:128], preferred_element_type=jnp.float32)
        product = first[:, 0:128] + (first[:, 128:256] + second)
        squares = jnp.sum(rows * rows, axis=1, keepdims=True)
        for j in range(CHUNK):
            to(j, product[8 * j : 8 * j + 8], jnp.broadcast_to(squares[8 * j : 8 * j + 8], (8, 128)))

    home = DEVS - CHUNK

    def keep_own(j, product, squares):
        own_part[j, 0] = product
        own_part[j, 1] = squares

    multiply(send[home:DEVS].reshape(CHUNK * 8, 1024), keep_own)
    part[DEVS - 1] = own_part[CHUNK - 1]
    for j in range(CHUNK - 1):
        remote(own_part.at[j], part.at[home + j], o_ssem, o_rsem, here.at(ORDER[home + j])).start()
    send_blocks(EARLY, DEVS - 1)

    inv_copy.wait()

    @pl.loop(0, DEVS, unroll=8)
    def _(p):
        here_s[p] = from_s[inv_s[0, p]]

    def arrived(i, count):
        v = recv.at[pl.ds(0, count)]
        remote(v, v, ssem, rsem.at[i], (row, col)).wait_recv()

    @pl.loop(0, CHUNKS - 1)
    def _(i):
        arrived(i, CHUNK)

        def keep(j, product, squares):
            part[i * CHUNK + j, 0] = product
            part[i * CHUNK + j, 1] = squares

        multiply(recv[pl.ds(i * CHUNK, CHUNK)].reshape(CHUNK * 8, 1024), keep)

    o7 = part.at[pl.ds(0, CHUNK - 1)]
    remote(o7, o7, o_ssem, o_rsem, (row, col)).wait()

    lane = lax.broadcasted_iota(jnp.int32, (8, 128), 1)
    sublane = lax.broadcasted_iota(jnp.int32, (8, 128), 0)
    diagonal = (lax.rem(lane, 8) == sublane) & (lane < 64)

    @pl.loop(0, COLS)
    def _(c):
        for t in range(2):
            tile = part[here_s[c * 8 + t * 4], 0]
            for i in range(1, 4):
                tile = jnp.where(lane < 32 * i, tile, part[here_s[c * 8 + t * 4 + i], 0])
            p_send[c, t] = tile
        tile = part[here_s[c * 8], 1]
        for i in range(1, 8):
            tile = jnp.where(lane < 8 * i, tile, part[here_s[c * 8 + i], 1])
        s_send[c] = jnp.sum(jnp.where(diagonal, tile, 0.0), axis=0, keepdims=True)

    across = [(0, b, z, k) for z in range(4) for b in range(2) for k in range(2) if (b, z, k) != (0, 0, 0)]
    for o in sorted(across, key=distance, reverse=True):
        c = here.z_col[o[2]] + here.y_col[o[1]] + here.core[o[3]]
        remote(p_send.at[c], p_recv.at[col], p_ssem, p_rsem, (row, c)).start()
        remote(s_send.at[c], s_recv.at[col], s_ssem, s_rsem, (row, c)).start()

    p_recv[col] = p_send[col]
    s_recv[col] = s_send[col]
    arrived(CHUNKS - 1, CHUNK - 1)

    @pl.loop(0, DEVS, unroll=8)
    def _(p):
        relaid[p] = recv[here_s[p]]

    p15 = p_recv.at[pl.ds(0, COLS - 1)]
    remote(p15, p15, p_ssem, p_rsem, (row, col)).wait()
    s15 = s_recv.at[pl.ds(0, COLS - 1)]
    remote(s15, s15, s_ssem, s_rsem, (row, col)).wait()
    v = recv.at[pl.ds(0, DEVS - 1)]
    remote(v, v, ssem, rsem.at[0], (row, col)).wait_send()


PIECES = 4


def finish(block, shares, squares, relaid, p_out, norm_out, sem):
    step = DEVS // PIECES
    copies = [
        pltpu.make_async_copy(block.at[pl.ds(i * step, step)], relaid.at[pl.ds(i * step, step)], sem.at[i])
        for i in range(PIECES)
    ]
    for copy in copies:
        copy.start()
    total, square = shares[0], squares[0]
    for c in range(1, COLS):
        total, square = total + shares[c], square + squares[c]
    norm_out[...] = jnp.sqrt(square[:, 0:64] / 16384.0 + epsilon)
    rows = []
    for g in range(8):
        t, i = divmod(g, 4)
        rows.append(total[t] if i == 0 else pltpu.roll(total[t], 128 - 32 * i, axis=1))
    p_out[...] = jnp.transpose(jnp.concatenate(rows + rows, axis=0))[0:32, 0:64]
    for copy in copies:
        copy.wait()


def on_device(old_residual, group_map, q_factor):
    f32, i32 = jnp.float32, jnp.int32
    hbm = pl.BlockSpec(memory_space=pltpu.HBM)
    vmem = pl.BlockSpec(memory_space=pltpu.VMEM)
    dma = pltpu.SemaphoreType.DMA
    given = [
        pltpu.with_memory_space_constraint(a, pltpu.HBM)
        for a in (old_residual.reshape(ROWS, 8, 16384), group_map.T, q_factor.T)
    ]
    block, shares, squares = pl.pallas_call(
        exchange,
        out_shape=(
            jax.ShapeDtypeStruct((DEVS, 8, 1024), f32),
            jax.ShapeDtypeStruct((COLS, 2, 8, 128), f32),
            jax.ShapeDtypeStruct((COLS, 1, 128), f32),
        ),
        in_specs=[hbm, hbm, hbm],
        out_specs=(vmem, vmem, vmem),
        scratch_shapes=[
            pltpu.VMEM((ROWS, 8, 16384), f32),
            pltpu.VMEM((DEVS, 8, 1024), f32),
            pltpu.VMEM((DEVS, 8, 1024), f32),
            pltpu.SMEM((8, 128), i32),
            pltpu.VMEM((8, 128), i32),
            pltpu.VMEM((4, 1024), f32),
            pltpu.VMEM((ROWS, 4, 1024), f32),
            pltpu.VMEM((128, 1024), f32),
            pltpu.VMEM((1024, 256), jnp.bfloat16),
            pltpu.VMEM((DEVS, 2, 8, 128), f32),
            pltpu.VMEM((CHUNK, 2, 8, 128), f32),
            pltpu.VMEM((COLS, 2, 8, 128), f32),
            pltpu.VMEM((COLS, 1, 128), f32),
            pltpu.VMEM((8, 128), i32),
            pltpu.SMEM((8, 128), i32),
            pltpu.SMEM((ROWS,), i32),
            pltpu.SMEM((DEVS,), i32),
            pltpu.SMEM((DEVS,), i32),
            dma((COLS,)),
            dma((2,)),
            dma,
            dma,
            dma,
            dma,
            dma,
            dma((CHUNKS,)),
            dma,
            dma,
            dma,
            dma,
            dma,
            dma,
        ],
        compiler_params=pltpu.CompilerParams(
            collective_id=0, has_side_effects=True, vmem_limit_bytes=40 << 20
        ),
    )(*given)
    relaid, projection, norms = pl.pallas_call(
        finish,
        out_shape=(
            jax.ShapeDtypeStruct((DEVS, 8, 1024), f32),
            jax.ShapeDtypeStruct((32, 64), f32),
            jax.ShapeDtypeStruct((1, 64), f32),
        ),
        in_specs=[vmem, vmem, vmem],
        out_specs=(hbm, vmem, vmem),
        scratch_shapes=[dma((PIECES,))],
        compiler_params=pltpu.CompilerParams(vmem_limit_bytes=16 << 20),
    )(block, shares, squares)
    return relaid.reshape(1024, 1024), projection, norms.reshape(64)


def solution(mesh):
    return jax.shard_map(
        on_device,
        mesh=mesh,
        in_specs=(P(("row", "col"), None), P(), P("col", "row")),
        out_specs=(P("row", "col"), P(None, ("row", "col")), P(("row", "col"))),
        check_vma=False,
    )
```

```python
import jax
import jax.numpy as jnp
from jax import lax
from jax.experimental import pallas as pl
from jax.experimental.pallas import tpu as pltpu
from jax.sharding import PartitionSpec as P

epsilon = 1e-06
MESH = pl.DeviceIdType.MESH
ROWS, COLS = 8, 16
DEVS = ROWS * COLS
BULK = DEVS - ROWS
CHUNK = 24
CHUNKS = BULK // CHUNK


def order():
    offsets = []
    for n in range(DEVS):
        c = 1 + MULT_C * n % 15 if n < DEVS - ROWS else 0
        s = MULT_S * (n + 1) % ROWS
        v = {name: c >> i & 1 for i, name in enumerate(BITS_C)} | {name: s >> i & 1 for i, name in enumerate(BITS_S)}
        offsets.append((v["x0"] + 2 * v["x1"], v["y0"] + 2 * v["y1"], v["z0"] + 2 * v["z1"], v["k"]))
    axes = lambda o: sum(1 for d in o[:3] if d)
    spread = lambda group, count: [group[len(group) * i // count] for i in range(count)]
    first = spread([o for o in offsets[: DEVS - ROWS] if axes(o) < 2], NEAR)
    second = spread([o for o in offsets[: DEVS - ROWS] if axes(o) == 2], PLANE)
    return first + second + [o for o in offsets if o not in first + second]


NEAR, PLANE = 15, 16
MULT_C, MULT_S = 7, 3
BITS_C, BITS_S = ("z0", "z1", "y0", "k"), ("x0", "x1", "y1")
EARLY = 96
ORDER = order()
HOPS = (0, 1, 2, 1)


class Place:
    def __init__(self):
        row, col = lax.axis_index("row"), lax.axis_index("col")
        x, z, core = lax.div(row, 2), lax.div(col, 4), lax.rem(col, 2)
        y = lax.rem(row, 2) * 2 + lax.rem(lax.div(col, 2), 2)
        ys = [lax.rem(y + d, 4) for d in range(4)]
        self.row, self.col, self.me = row, col, row * COLS + col
        self.x_row = [2 * lax.rem(x + d, 4) for d in range(4)]
        self.y_row = [lax.div(v, 2) for v in ys]
        self.y_col = [2 * lax.rem(v, 2) for v in ys]
        self.z_col = [4 * lax.rem(z + d, 4) for d in range(4)]
        self.core = [core, 1 - core]

    def at(self, o):
        return self.x_row[o[0]] + self.y_row[o[1]], self.z_col[o[2]] + self.y_col[o[1]] + self.core[o[3]]

    def back(self, o):
        row, col = self.at((-o[0] % 4, -o[1] % 4, -o[2] % 4, o[3]))
        return row * COLS + col


def distance(o):
    return HOPS[o[0]] + HOPS[o[1]] + HOPS[o[2]] + 0.25 * o[3]


def exchange(
    old, ids, q_own, relaid, p_recv, s_recv,
    stage, send, recv, ids_s, ids_v, q_mine, q_all, w_rows, w, part, p_send, s_send,
    inv_v, inv_s, slot_s, from_s, here_s,
    in_sem, ids_sem, inv_sem, q_sem, q_ssem, q_rsem, ssem, rsem, p_ssem, p_rsem, s_ssem, s_rsem, tree,
):
    here = Place()
    row, col, me = here.row, here.col, here.me

    def remote(src, dst, send_sem, recv_sem, to):
        return pltpu.make_async_remote_copy(
            src_ref=src, dst_ref=dst, send_sem=send_sem, recv_sem=recv_sem, device_id=to, device_id_type=MESH
        )

    ids_copy = pltpu.make_async_copy(ids, ids_s, ids_sem.at[0])
    ids_copy2 = pltpu.make_async_copy(ids, ids_v, ids_sem.at[1])
    q_copy = pltpu.make_async_copy(q_own, q_mine, q_sem)
    ids_copy.start()
    loads = []
    for j in range(ROWS):
        loads.append(pltpu.make_async_copy(old.at[j], stage.at[j], in_sem.at[j]))
        loads[-1].start()
    q_copy.start()
    ids_copy2.start()

    barrier = pltpu.get_barrier_semaphore()
    lines = [(d, 0, 0, k) for d in range(4) for k in range(2) if d or k]
    lines += [(0, d, 0, k) for d in range(1, 4) for k in range(2)]
    lines += [(0, 0, d, k) for d in range(1, 4) for k in range(2)]
    for o in sorted(lines, key=distance, reverse=True):
        pl.semaphore_signal(barrier, inc=1, device_id=here.at(o), device_id_type=MESH)

    pl.semaphore_wait(barrier, len(lines))
    for d in (2, 1, 3):
        pl.semaphore_signal(tree.at[0], inc=1, device_id=here.at((d, 0, 0, 0)), device_id_type=MESH)
        pl.semaphore_signal(tree.at[0], inc=1, device_id=here.at((0, d, 0, 0)), device_id_type=MESH)
    ids_copy.wait()
    for k in range(ROWS):
        slot = jnp.int32(0)
        for j in range(ROWS):
            slot += jnp.where(lax.shift_right_arithmetic(ids_s[j, me], 7) == k, j, 0)
        slot_s[k] = lax.bitwise_and(slot, 7)

    for load in loads:
        load.wait()

    def arrange(first, last):
        for n in range(first, last):
            r, c = here.at(ORDER[n])
            send[n] = stage[slot_s[r], :, pl.ds(pl.multiple_of(c * 1024, 1024), 1024)]

    arrange(0, NEAR)

    def send_blocks(first, last):
        for n in range(first, last):
            remote(send.at[n], recv.at[n], ssem, rsem.at[min(n // CHUNK, CHUNKS)], here.at(ORDER[n])).start()

    q_copy.wait()
    remote(q_mine, q_all.at[row], q_ssem, q_rsem.at[0], here.at((0, 2, 0, 0))).start()
    for d in (2, 1, 3):
        remote(q_mine, q_all.at[row], q_ssem, q_rsem.at[1], here.at((d, 0, 0, 0))).start()
    send_blocks(0, NEAR)
    arrange(NEAR, DEVS)
    pl.semaphore_wait(tree.at[0], 6)
    for d in (2, 1, 3):
        pl.semaphore_signal(tree.at[1], inc=1, device_id=here.at((d, 0, 0, 0)), device_id_type=MESH)
    send_blocks(NEAR, NEAR + PLANE)
    partner = here.at((0, 2, 0, 0))[0]
    remote(q_mine, q_all.at[partner], q_ssem, q_rsem.at[0], (row, col)).wait_recv()
    for d in (2, 1, 3):
        remote(q_all.at[partner], q_all.at[partner], q_ssem, q_rsem.at[2], here.at((d, 0, 0, 0))).start()
    pl.semaphore_wait(tree.at[1], 3)
    send_blocks(NEAR + PLANE, EARLY)
    send_blocks(EARLY, DEVS - 1)

    q_all[row] = q_mine[...]
    recv[DEVS - 1] = send[DEVS - 1]

    ids_copy2.wait()
    held = ids_v[...]
    mine = lax.shift_right_arithmetic(held, 7) == row
    where_to = jnp.sum(jnp.where(mine, lax.bitwise_and(held, 127), 0), axis=0, keepdims=True)
    spread = jnp.transpose(jnp.broadcast_to(where_to, (DEVS, DEVS)))
    lanes = lax.broadcasted_iota(jnp.int32, (DEVS, DEVS), 1)
    sources = lax.broadcasted_iota(jnp.int32, (DEVS, DEVS), 0)
    inverse = jnp.sum(jnp.where(spread == lanes, sources, 0), axis=0, keepdims=True)
    inv_v[...] = jnp.broadcast_to(lax.bitwise_and(inverse, 127), (8, DEVS))
    inv_copy = pltpu.make_async_copy(inv_v, inv_s, inv_sem)
    inv_copy.start()
    for n, o in enumerate(ORDER):
        from_s[here.back(o)] = n

    q7, q3 = q_all.at[pl.ds(0, ROWS - 1)], q_all.at[pl.ds(0, 3)]
    remote(q3, q3, q_ssem, q_rsem.at[1], (row, col)).wait_recv()
    remote(q3, q3, q_ssem, q_rsem.at[2], (row, col)).wait_recv()
    remote(q7, q7, q_ssem, q_rsem.at[2], (row, col)).wait_send()
    for r in range(ROWS):
        for i in range(4):
            w_rows[32 * i + 4 * r : 32 * i + 4 * r + 4, :] = q_all[r]
    w_all = jnp.transpose(w_rows[...])
    w_high = w_all.astype(jnp.bfloat16)
    w[:, 0:128] = w_high
    w[:, 128:256] = (w_all - w_high.astype(jnp.float32)).astype(jnp.bfloat16)

    def multiply(rows, to):
        high = rows.astype(jnp.bfloat16)
        low = (rows - high.astype(jnp.float32)).astype(jnp.bfloat16)
        first = jnp.dot(high, w[...], preferred_element_type=jnp.float32)
        second = jnp.dot(low, w[:, 0:128], preferred_element_type=jnp.float32)
        product = first[:, 0:128] + (first[:, 128:256] + second)
        squares = jnp.sum(rows * rows, axis=1, keepdims=True)
        for j in range(rows.shape[0] // 8):
            to(j, product[8 * j : 8 * j + 8], jnp.broadcast_to(squares[8 * j : 8 * j + 8], (8, 128)))

    inv_copy.wait()

    @pl.loop(0, DEVS, unroll=8)
    def _(p):
        here_s[p] = from_s[inv_s[0, p]]

    def arrived(i, count):
        v = recv.at[pl.ds(0, count)]
        remote(v, v, ssem, rsem.at[i], (row, col)).wait_recv()

    def product(first, count):
        def keep(j, product, squares):
            part[first + j, 0] = product
            part[first + j, 1] = squares

        multiply(recv[pl.ds(first, count)].reshape(count * 8, 1024), keep)

    @pl.loop(0, CHUNKS)
    def _(i):
        arrived(i, CHUNK)
        product(i * CHUNK, CHUNK)

    arrived(CHUNKS, ROWS - 1)
    product(BULK, ROWS)

    lane = lax.broadcasted_iota(jnp.int32, (8, 128), 1)
    sublane = lax.broadcasted_iota(jnp.int32, (8, 128), 0)
    diagonal = (lax.rem(lane, 8) == sublane) & (lane < 64)

    def gather(c, p_to, s_to):
        for t in range(2):
            tile = part[here_s[c * 8 + t * 4], 0]
            for i in range(1, 4):
                tile = jnp.where(lane < 32 * i, tile, part[here_s[c * 8 + t * 4 + i], 0])
            p_to[t] = tile
        tile = part[here_s[c * 8], 1]
        for i in range(1, 8):
            tile = jnp.where(lane < 8 * i, tile, part[here_s[c * 8 + i], 1])
        s_to[...] = jnp.sum(jnp.where(diagonal, tile, 0.0), axis=0, keepdims=True)

    across = [(0, b, z, k) for z in range(4) for b in range(2) for k in range(2) if (b, z, k) != (0, 0, 0)]
    across = sorted(across, key=distance, reverse=True)

    def column(o):
        return here.z_col[o[2]] + here.y_col[o[1]] + here.core[o[3]]

    def share(some):
        for o in some:
            c = column(o)
            remote(p_send.at[c], p_recv.at[col], p_ssem, p_rsem, (row, c)).start()
            remote(s_send.at[c], s_recv.at[col], s_ssem, s_rsem, (row, c)).start()

    for first in range(0, 16, 4):
        for o in across[first : first + 4]:
            gather(column(o), p_send.at[column(o)], s_send.at[column(o)])
        if first:
            share(across[first - 4 : first])
    share(across[12:])
    gather(col, p_recv.at[col], s_recv.at[col])

    @pl.loop(0, DEVS, unroll=8)
    def _(p):
        relaid[p] = recv[here_s[p]]

    p15 = p_recv.at[pl.ds(0, COLS - 1)]
    remote(p15, p15, p_ssem, p_rsem, (row, col)).wait()
    s15 = s_recv.at[pl.ds(0, COLS - 1)]
    remote(s15, s15, s_ssem, s_rsem, (row, col)).wait()
    v = recv.at[pl.ds(0, DEVS - 1)]
    remote(v, v, ssem, rsem.at[0], (row, col)).wait_send()


PIECES = 4


def finish(block, shares, squares, relaid, p_out, norm_out, p_done, norm_done, sem, small_sem):
    step = DEVS // PIECES
    copies = [
        pltpu.make_async_copy(block.at[pl.ds(i * step, step)], relaid.at[pl.ds(i * step, step)], sem.at[i])
        for i in range(PIECES)
    ]
    for copy in copies:
        copy.start()
    total, square = shares[0], squares[0]
    for c in range(1, COLS):
        total, square = total + shares[c], square + squares[c]
    norm_done[...] = jnp.sqrt(square[:, 0:64] / 16384.0 + epsilon)
    rows = []
    for g in range(8):
        t, i = divmod(g, 4)
        rows.append(total[t] if i == 0 else pltpu.roll(total[t], 128 - 32 * i, axis=1))
    p_done[...] = jnp.transpose(jnp.concatenate(rows + rows, axis=0))[0:32, 0:64]
    small = [
        pltpu.make_async_copy(norm_done, norm_out, small_sem.at[0]),
        pltpu.make_async_copy(p_done, p_out, small_sem.at[1]),
    ]
    for copy in small:
        copy.start()
    for copy in copies + small:
        copy.wait()


def on_device(old_residual, group_map, q_factor):
    f32, i32 = jnp.float32, jnp.int32
    hbm = pl.BlockSpec(memory_space=pltpu.HBM)
    vmem = pl.BlockSpec(memory_space=pltpu.VMEM)
    dma = pltpu.SemaphoreType.DMA
    given = [
        pltpu.with_memory_space_constraint(a, pltpu.HBM)
        for a in (old_residual.reshape(ROWS, 8, 16384), group_map.T, q_factor.T)
    ]
    block, shares, squares = pl.pallas_call(
        exchange,
        out_shape=(
            jax.ShapeDtypeStruct((DEVS, 8, 1024), f32),
            jax.ShapeDtypeStruct((COLS, 2, 8, 128), f32),
            jax.ShapeDtypeStruct((COLS, 1, 128), f32),
        ),
        in_specs=[hbm, hbm, hbm],
        out_specs=(vmem, vmem, vmem),
        scratch_shapes=[
            pltpu.VMEM((ROWS, 8, 16384), f32),
            pltpu.VMEM((DEVS, 8, 1024), f32),
            pltpu.VMEM((DEVS, 8, 1024), f32),
            pltpu.SMEM((8, 128), i32),
            pltpu.VMEM((8, 128), i32),
            pltpu.VMEM((4, 1024), f32),
            pltpu.VMEM((ROWS, 4, 1024), f32),
            pltpu.VMEM((128, 1024), f32),
            pltpu.VMEM((1024, 256), jnp.bfloat16),
            pltpu.VMEM((DEVS, 2, 8, 128), f32),
            pltpu.VMEM((COLS, 2, 8, 128), f32),
            pltpu.VMEM((COLS, 1, 128), f32),
            pltpu.VMEM((8, 128), i32),
            pltpu.SMEM((8, 128), i32),
            pltpu.SMEM((ROWS,), i32),
            pltpu.SMEM((DEVS,), i32),
            pltpu.SMEM((DEVS,), i32),
            dma((COLS,)),
            dma((2,)),
            dma,
            dma,
            dma,
            dma((3,)),
            dma,
            dma((CHUNKS + 1,)),
            dma,
            dma,
            dma,
            dma,
            pltpu.SemaphoreType.REGULAR((2,)),
        ],
        compiler_params=pltpu.CompilerParams(
            collective_id=0, has_side_effects=True, vmem_limit_bytes=40 << 20
        ),
    )(*given)
    relaid, projection, norms = pl.pallas_call(
        finish,
        out_shape=(
            jax.ShapeDtypeStruct((DEVS, 8, 1024), f32),
            jax.ShapeDtypeStruct((32, 64), f32),
            jax.ShapeDtypeStruct((1, 64), f32),
        ),
        in_specs=[vmem, vmem, vmem],
        out_specs=(hbm, hbm, hbm),
        scratch_shapes=[pltpu.VMEM((32, 64), f32), pltpu.VMEM((1, 64), f32), dma((PIECES,)), dma((2,))],
        compiler_params=pltpu.CompilerParams(vmem_limit_bytes=16 << 20),
    )(block, shares, squares)
    return relaid.reshape(1024, 1024), projection, norms.reshape(64)


def solution(mesh):
    return jax.shard_map(
        on_device,
        mesh=mesh,
        in_specs=(P(("row", "col"), None), P(), P("col", "row")),
        out_specs=(P("row", "col"), P(None, ("row", "col")), P(("row", "col"))),
        check_vma=False,
    )
```

```python
import jax
import jax.numpy as jnp
from jax import lax
from jax.experimental import pallas as pl
from jax.experimental.pallas import tpu as pltpu
from jax.sharding import PartitionSpec as P

epsilon = 1e-06
MESH = pl.DeviceIdType.MESH
ROWS, COLS = 8, 16
DEVS = ROWS * COLS
BULK = DEVS - ROWS
CHUNK = 24
CHUNKS = BULK // CHUNK


def order():
    offsets = []
    for n in range(DEVS):
        c = 1 + MULT_C * n % 15 if n < DEVS - ROWS else 0
        s = MULT_S * (n + 1) % ROWS
        v = {name: c >> i & 1 for i, name in enumerate(BITS_C)} | {name: s >> i & 1 for i, name in enumerate(BITS_S)}
        offsets.append((v["x0"] + 2 * v["x1"], v["y0"] + 2 * v["y1"], v["z0"] + 2 * v["z1"], v["k"]))
    axes = lambda o: sum(1 for d in o[:3] if d)
    spread = lambda group, count: [group[len(group) * i // count] for i in range(count)]
    first = spread([o for o in offsets[: DEVS - ROWS] if axes(o) < 2], NEAR)
    second = spread([o for o in offsets[: DEVS - ROWS] if axes(o) == 2], PLANE)
    rest = [o for o in offsets[: DEVS - ROWS] if o not in first + second]
    far = lambda o: -sum((0, 1, 2, 1)[d] for d in o[:3])
    return first + second + rest[:-12] + sorted(rest[-12:], key=far) + sorted(offsets[DEVS - ROWS :], key=far)


NEAR, PLANE = 15, 12
MULT_C, MULT_S = 7, 3
BITS_C, BITS_S = ("z0", "z1", "y0", "k"), ("x0", "x1", "y1")
EARLY = 96
ORDER = order()
HOPS = (0, 1, 2, 1)


class Place:
    def __init__(self):
        row, col = lax.axis_index("row"), lax.axis_index("col")
        x, z, core = lax.div(row, 2), lax.div(col, 4), lax.rem(col, 2)
        y = lax.rem(row, 2) * 2 + lax.rem(lax.div(col, 2), 2)
        ys = [lax.rem(y + d, 4) for d in range(4)]
        self.row, self.col, self.me = row, col, row * COLS + col
        self.x_row = [2 * lax.rem(x + d, 4) for d in range(4)]
        self.y_row = [lax.div(v, 2) for v in ys]
        self.y_col = [2 * lax.rem(v, 2) for v in ys]
        self.z_col = [4 * lax.rem(z + d, 4) for d in range(4)]
        self.core = [core, 1 - core]

    def at(self, o):
        return self.x_row[o[0]] + self.y_row[o[1]], self.z_col[o[2]] + self.y_col[o[1]] + self.core[o[3]]

    def back(self, o):
        row, col = self.at((-o[0] % 4, -o[1] % 4, -o[2] % 4, o[3]))
        return row * COLS + col


def distance(o):
    return HOPS[o[0]] + HOPS[o[1]] + HOPS[o[2]] + 0.25 * o[3]


def exchange(
    old, ids, q_own, relaid, p_recv, s_recv,
    stage, send, recv, ids_s, ids_v, q_mine, q_all, w_rows, w, part, p_send, s_send,
    inv_v, inv_s, slot_s, from_s, here_s,
    in_sem, ids_sem, inv_sem, q_sem, q_ssem, q_rsem, ssem, rsem, p_ssem, p_rsem, s_ssem, s_rsem, tree,
):
    here = Place()
    row, col, me = here.row, here.col, here.me

    def remote(src, dst, send_sem, recv_sem, to):
        return pltpu.make_async_remote_copy(
            src_ref=src, dst_ref=dst, send_sem=send_sem, recv_sem=recv_sem, device_id=to, device_id_type=MESH
        )

    ids_copy = pltpu.make_async_copy(ids, ids_s, ids_sem.at[0])
    ids_copy2 = pltpu.make_async_copy(ids, ids_v, ids_sem.at[1])
    q_copy = pltpu.make_async_copy(q_own, q_mine, q_sem)
    ids_copy.start()
    loads = []
    for j in range(ROWS):
        loads.append(pltpu.make_async_copy(old.at[j], stage.at[j], in_sem.at[j]))
        loads[-1].start()
    q_copy.start()
    ids_copy2.start()

    barrier = pltpu.get_barrier_semaphore()
    lines = [(d, 0, 0, k) for d in range(4) for k in range(2) if d or k]
    lines += [(0, d, 0, k) for d in range(1, 4) for k in range(2)]
    lines += [(0, 0, d, k) for d in range(1, 4) for k in range(2)]
    for o in sorted(lines, key=distance, reverse=True):
        pl.semaphore_signal(barrier, inc=1, device_id=here.at(o), device_id_type=MESH)

    pl.semaphore_wait(barrier, len(lines))
    for d in (2, 1, 3):
        pl.semaphore_signal(tree.at[0], inc=1, device_id=here.at((d, 0, 0, 0)), device_id_type=MESH)
        pl.semaphore_signal(tree.at[0], inc=1, device_id=here.at((0, d, 0, 0)), device_id_type=MESH)
    ids_copy.wait()
    for k in range(ROWS):
        slot = jnp.int32(0)
        for j in range(ROWS):
            slot += jnp.where(lax.shift_right_arithmetic(ids_s[j, me], 7) == k, j, 0)
        slot_s[k] = lax.bitwise_and(slot, 7)

    for load in loads:
        load.wait()

    def arrange(first, last):
        for n in range(first, last):
            r, c = here.at(ORDER[n])
            send[n] = stage[slot_s[r], :, pl.ds(pl.multiple_of(c * 1024, 1024), 1024)]

    arrange(0, NEAR)

    def send_blocks(first, last):
        for n in range(first, last):
            remote(send.at[n], recv.at[n], ssem, rsem.at[min(n // CHUNK, CHUNKS)], here.at(ORDER[n])).start()

    q_copy.wait()
    remote(q_mine, q_all.at[row], q_ssem, q_rsem.at[0], here.at((0, 2, 0, 0))).start()
    for d in (2, 1, 3):
        remote(q_mine, q_all.at[row], q_ssem, q_rsem.at[1], here.at((d, 0, 0, 0))).start()
    send_blocks(0, NEAR)
    arrange(NEAR, DEVS)
    pl.semaphore_wait(tree.at[0], 6)
    for d in (2, 1, 3):
        pl.semaphore_signal(tree.at[1], inc=1, device_id=here.at((d, 0, 0, 0)), device_id_type=MESH)
    send_blocks(NEAR, NEAR + PLANE)
    partner = here.at((0, 2, 0, 0))[0]
    remote(q_mine, q_all.at[partner], q_ssem, q_rsem.at[0], (row, col)).wait_recv()
    for d in (2, 1, 3):
        remote(q_all.at[partner], q_all.at[partner], q_ssem, q_rsem.at[2], here.at((d, 0, 0, 0))).start()
    pl.semaphore_wait(tree.at[1], 3)
    send_blocks(NEAR + PLANE, EARLY)
    send_blocks(EARLY, DEVS - 1)

    q_all[row] = q_mine[...]
    recv[DEVS - 1] = send[DEVS - 1]

    ids_copy2.wait()
    held = ids_v[...]
    mine = lax.shift_right_arithmetic(held, 7) == row
    where_to = jnp.sum(jnp.where(mine, lax.bitwise_and(held, 127), 0), axis=0, keepdims=True)
    spread = jnp.transpose(jnp.broadcast_to(where_to, (DEVS, DEVS)))
    lanes = lax.broadcasted_iota(jnp.int32, (DEVS, DEVS), 1)
    sources = lax.broadcasted_iota(jnp.int32, (DEVS, DEVS), 0)
    inverse = jnp.sum(jnp.where(spread == lanes, sources, 0), axis=0, keepdims=True)
    inv_v[...] = jnp.broadcast_to(lax.bitwise_and(inverse, 127), (8, DEVS))
    inv_copy = pltpu.make_async_copy(inv_v, inv_s, inv_sem)
    inv_copy.start()
    for n, o in enumerate(ORDER):
        from_s[here.back(o)] = n

    q7, q3 = q_all.at[pl.ds(0, ROWS - 1)], q_all.at[pl.ds(0, 3)]
    remote(q3, q3, q_ssem, q_rsem.at[1], (row, col)).wait_recv()
    remote(q3, q3, q_ssem, q_rsem.at[2], (row, col)).wait_recv()
    remote(q7, q7, q_ssem, q_rsem.at[2], (row, col)).wait_send()
    for r in range(ROWS):
        for i in range(4):
            w_rows[32 * i + 4 * r : 32 * i + 4 * r + 4, :] = q_all[r]
    w_all = jnp.transpose(w_rows[...])
    w_high = w_all.astype(jnp.bfloat16)
    w[:, 0:128] = w_high
    w[:, 128:256] = (w_all - w_high.astype(jnp.float32)).astype(jnp.bfloat16)

    def multiply(rows, to):
        high = rows.astype(jnp.bfloat16)
        low = (rows - high.astype(jnp.float32)).astype(jnp.bfloat16)
        first = jnp.dot(high, w[...], preferred_element_type=jnp.float32)
        second = jnp.dot(low, w[:, 0:128], preferred_element_type=jnp.float32)
        product = first[:, 0:128] + (first[:, 128:256] + second)
        squares = jnp.sum(rows * rows, axis=1, keepdims=True)
        for j in range(rows.shape[0] // 8):
            to(j, product[8 * j : 8 * j + 8], jnp.broadcast_to(squares[8 * j : 8 * j + 8], (8, 128)))

    inv_copy.wait()

    @pl.loop(0, DEVS, unroll=8)
    def _(p):
        here_s[p] = from_s[inv_s[0, p]]

    def arrived(i, count):
        v = recv.at[pl.ds(0, count)]
        remote(v, v, ssem, rsem.at[i], (row, col)).wait_recv()

    def product(first, count):
        def keep(j, product, squares):
            part[first + j, 0] = product
            part[first + j, 1] = squares

        multiply(recv[pl.ds(first, count)].reshape(count * 8, 1024), keep)

    @pl.loop(0, CHUNKS)
    def _(i):
        arrived(i, CHUNK)
        product(i * CHUNK, CHUNK)

    arrived(CHUNKS, ROWS - 1)
    product(BULK, ROWS)

    lane = lax.broadcasted_iota(jnp.int32, (8, 128), 1)
    sublane = lax.broadcasted_iota(jnp.int32, (8, 128), 0)
    diagonal = (lax.rem(lane, 8) == sublane) & (lane < 64)

    def gather(c, p_to, s_to):
        for t in range(2):
            tile = part[here_s[c * 8 + t * 4], 0]
            for i in range(1, 4):
                tile = jnp.where(lane < 32 * i, tile, part[here_s[c * 8 + t * 4 + i], 0])
            p_to[t] = tile
        tile = part[here_s[c * 8], 1]
        for i in range(1, 8):
            tile = jnp.where(lane < 8 * i, tile, part[here_s[c * 8 + i], 1])
        s_to[...] = jnp.sum(jnp.where(diagonal, tile, 0.0), axis=0, keepdims=True)

    across = [(0, b, z, k) for z in range(4) for b in range(2) for k in range(2) if (b, z, k) != (0, 0, 0)]
    across = sorted(across, key=distance, reverse=True)

    def column(o):
        return here.z_col[o[2]] + here.y_col[o[1]] + here.core[o[3]]

    def share(some):
        for o in some:
            c = column(o)
            remote(p_send.at[c], p_recv.at[col], p_ssem, p_rsem, (row, c)).start()
            remote(s_send.at[c], s_recv.at[col], s_ssem, s_rsem, (row, c)).start()

    for first in range(0, 16, 4):
        for o in across[first : first + 4]:
            gather(column(o), p_send.at[column(o)], s_send.at[column(o)])
        if first:
            share(across[first - 4 : first])
    share(across[12:])
    gather(col, p_recv.at[col], s_recv.at[col])

    @pl.loop(0, DEVS, unroll=8)
    def _(p):
        relaid[p] = recv[here_s[p]]

    p15 = p_recv.at[pl.ds(0, COLS - 1)]
    remote(p15, p15, p_ssem, p_rsem, (row, col)).wait()
    s15 = s_recv.at[pl.ds(0, COLS - 1)]
    remote(s15, s15, s_ssem, s_rsem, (row, col)).wait()
    v = recv.at[pl.ds(0, DEVS - 1)]
    remote(v, v, ssem, rsem.at[0], (row, col)).wait_send()


PIECES = 4


def finish(block, shares, squares, relaid, p_out, norm_out, p_done, norm_done, sem, small_sem):
    step = DEVS // PIECES
    copies = [
        pltpu.make_async_copy(block.at[pl.ds(i * step, step)], relaid.at[pl.ds(i * step, step)], sem.at[i])
        for i in range(PIECES)
    ]
    for copy in copies:
        copy.start()
    total, square = shares[0], squares[0]
    for c in range(1, COLS):
        total, square = total + shares[c], square + squares[c]
    norm_done[...] = jnp.sqrt(square[:, 0:64] / 16384.0 + epsilon)
    rows = []
    for g in range(8):
        t, i = divmod(g, 4)
        rows.append(total[t] if i == 0 else pltpu.roll(total[t], 128 - 32 * i, axis=1))
    p_done[...] = jnp.transpose(jnp.concatenate(rows + rows, axis=0))[0:32, 0:64]
    small = [
        pltpu.make_async_copy(norm_done, norm_out, small_sem.at[0]),
        pltpu.make_async_copy(p_done, p_out, small_sem.at[1]),
    ]
    for copy in small:
        copy.start()
    for copy in copies + small:
        copy.wait()


def on_device(old_residual, group_map, q_factor):
    f32, i32 = jnp.float32, jnp.int32
    hbm = pl.BlockSpec(memory_space=pltpu.HBM)
    vmem = pl.BlockSpec(memory_space=pltpu.VMEM)
    dma = pltpu.SemaphoreType.DMA
    given = [
        pltpu.with_memory_space_constraint(a, pltpu.HBM)
        for a in (old_residual.reshape(ROWS, 8, 16384), group_map.T, q_factor.T)
    ]
    block, shares, squares = pl.pallas_call(
        exchange,
        out_shape=(
            jax.ShapeDtypeStruct((DEVS, 8, 1024), f32),
            jax.ShapeDtypeStruct((COLS, 2, 8, 128), f32),
            jax.ShapeDtypeStruct((COLS, 1, 128), f32),
        ),
        in_specs=[hbm, hbm, hbm],
        out_specs=(vmem, vmem, vmem),
        scratch_shapes=[
            pltpu.VMEM((ROWS, 8, 16384), f32),
            pltpu.VMEM((DEVS, 8, 1024), f32),
            pltpu.VMEM((DEVS, 8, 1024), f32),
            pltpu.SMEM((8, 128), i32),
            pltpu.VMEM((8, 128), i32),
            pltpu.VMEM((4, 1024), f32),
            pltpu.VMEM((ROWS, 4, 1024), f32),
            pltpu.VMEM((128, 1024), f32),
            pltpu.VMEM((1024, 256), jnp.bfloat16),
            pltpu.VMEM((DEVS, 2, 8, 128), f32),
            pltpu.VMEM((COLS, 2, 8, 128), f32),
            pltpu.VMEM((COLS, 1, 128), f32),
            pltpu.VMEM((8, 128), i32),
            pltpu.SMEM((8, 128), i32),
            pltpu.SMEM((ROWS,), i32),
            pltpu.SMEM((DEVS,), i32),
            pltpu.SMEM((DEVS,), i32),
            dma((COLS,)),
            dma((2,)),
            dma,
            dma,
            dma,
            dma((3,)),
            dma,
            dma((CHUNKS + 1,)),
            dma,
            dma,
            dma,
            dma,
            pltpu.SemaphoreType.REGULAR((2,)),
        ],
        compiler_params=pltpu.CompilerParams(
            collective_id=0, has_side_effects=True, vmem_limit_bytes=40 << 20
        ),
    )(*given)
    relaid, projection, norms = pl.pallas_call(
        finish,
        out_shape=(
            jax.ShapeDtypeStruct((DEVS, 8, 1024), f32),
            jax.ShapeDtypeStruct((32, 64), f32),
            jax.ShapeDtypeStruct((1, 64), f32),
        ),
        in_specs=[vmem, vmem, vmem],
        out_specs=(hbm, hbm, hbm),
        scratch_shapes=[pltpu.VMEM((32, 64), f32), pltpu.VMEM((1, 64), f32), dma((PIECES,)), dma((2,))],
        compiler_params=pltpu.CompilerParams(vmem_limit_bytes=16 << 20),
    )(block, shares, squares)
    return relaid.reshape(1024, 1024), projection, norms.reshape(64)


def solution(mesh):
    return jax.shard_map(
        on_device,
        mesh=mesh,
        in_specs=(P(("row", "col"), None), P(), P("col", "row")),
        out_specs=(P("row", "col"), P(None, ("row", "col")), P(("row", "col"))),
        check_vma=False,
    )
```

```python
import jax
import jax.numpy as jnp
from jax import lax
from jax.experimental import pallas as pl
from jax.experimental.pallas import tpu as pltpu
from jax.sharding import PartitionSpec as P

epsilon = 1e-06
MESH = pl.DeviceIdType.MESH
ROWS, COLS = 8, 16
DEVS = ROWS * COLS
BULK = DEVS - ROWS
CHUNK = 8
CHUNKS = BULK // CHUNK


def order():
    offsets = []
    for n in range(DEVS):
        c = 1 + MULT_C * n % 15 if n < DEVS - ROWS else 0
        s = MULT_S * (n + 1) % ROWS
        v = {name: c >> i & 1 for i, name in enumerate(BITS_C)} | {name: s >> i & 1 for i, name in enumerate(BITS_S)}
        offsets.append((v["x0"] + 2 * v["x1"], v["y0"] + 2 * v["y1"], v["z0"] + 2 * v["z1"], v["k"]))
    axes = lambda o: sum(1 for d in o[:3] if d)
    spread = lambda group, count: [group[len(group) * i // count] for i in range(count)]
    first = spread([o for o in offsets[: DEVS - ROWS] if axes(o) < 2], NEAR)
    second = spread([o for o in offsets[: DEVS - ROWS] if axes(o) == 2], PLANE)
    rest = [o for o in offsets[: DEVS - ROWS] if o not in first + second]
    far = lambda o: -sum((0, 1, 2, 1)[d] for d in o[:3])
    return first + second + rest[:-12] + sorted(rest[-12:], key=far) + sorted(offsets[DEVS - ROWS :], key=far)


NEAR, PLANE = 15, 12
MULT_C, MULT_S = 7, 3
BITS_C, BITS_S = ("z0", "z1", "y0", "k"), ("x0", "x1", "y1")
EARLY = 96
ORDER = order()
HOPS = (0, 1, 2, 1)


class Place:
    def __init__(self):
        row, col = lax.axis_index("row"), lax.axis_index("col")
        x, z, core = lax.div(row, 2), lax.div(col, 4), lax.rem(col, 2)
        y = lax.rem(row, 2) * 2 + lax.rem(lax.div(col, 2), 2)
        ys = [lax.rem(y + d, 4) for d in range(4)]
        self.row, self.col, self.me = row, col, row * COLS + col
        self.x_row = [2 * lax.rem(x + d, 4) for d in range(4)]
        self.y_row = [lax.div(v, 2) for v in ys]
        self.y_col = [2 * lax.rem(v, 2) for v in ys]
        self.z_col = [4 * lax.rem(z + d, 4) for d in range(4)]
        self.core = [core, 1 - core]

    def at(self, o):
        return self.x_row[o[0]] + self.y_row[o[1]], self.z_col[o[2]] + self.y_col[o[1]] + self.core[o[3]]

    def back(self, o):
        row, col = self.at((-o[0] % 4, -o[1] % 4, -o[2] % 4, o[3]))
        return row * COLS + col


def distance(o):
    return HOPS[o[0]] + HOPS[o[1]] + HOPS[o[2]] + 0.25 * o[3]


def exchange(
    old, ids, q_own, relaid, p_recv, s_recv,
    stage, send, recv, ids_s, ids_v, q_mine, q_all, w_rows, w, part, own_part, own_recv, p_send, s_send,
    inv_v, inv_s, slot_s, from_s, here_s,
    in_sem, ids_sem, inv_sem, q_sem, q_ssem, q_rsem, ssem, rsem, o_ssem, o_rsem, p_ssem, p_rsem, s_ssem, s_rsem, tree,
):
    here = Place()
    row, col, me = here.row, here.col, here.me

    def remote(src, dst, send_sem, recv_sem, to):
        return pltpu.make_async_remote_copy(
            src_ref=src, dst_ref=dst, send_sem=send_sem, recv_sem=recv_sem, device_id=to, device_id_type=MESH
        )

    ids_copy = pltpu.make_async_copy(ids, ids_s, ids_sem.at[0])
    ids_copy2 = pltpu.make_async_copy(ids, ids_v, ids_sem.at[1])
    q_copy = pltpu.make_async_copy(q_own, q_mine, q_sem)
    ids_copy.start()
    loads = []
    for j in range(ROWS):
        loads.append(pltpu.make_async_copy(old.at[j], stage.at[j], in_sem.at[j]))
        loads[-1].start()
    q_copy.start()
    ids_copy2.start()

    barrier = pltpu.get_barrier_semaphore()
    lines = [(d, 0, 0, k) for d in range(4) for k in range(2) if d or k]
    lines += [(0, d, 0, k) for d in range(1, 4) for k in range(2)]
    lines += [(0, 0, d, k) for d in range(1, 4) for k in range(2)]
    for o in sorted(lines, key=distance, reverse=True):
        pl.semaphore_signal(barrier, inc=1, device_id=here.at(o), device_id_type=MESH)

    pl.semaphore_wait(barrier, len(lines))
    for d in (2, 1, 3):
        pl.semaphore_signal(tree.at[0], inc=1, device_id=here.at((d, 0, 0, 0)), device_id_type=MESH)
        pl.semaphore_signal(tree.at[0], inc=1, device_id=here.at((0, d, 0, 0)), device_id_type=MESH)
    ids_copy.wait()
    for k in range(ROWS):
        slot = jnp.int32(0)
        for j in range(ROWS):
            slot += jnp.where(lax.shift_right_arithmetic(ids_s[j, me], 7) == k, j, 0)
        slot_s[k] = lax.bitwise_and(slot, 7)

    for load in loads:
        load.wait()

    def arrange(first, last):
        for n in range(first, last):
            r, c = here.at(ORDER[n])
            send[n] = stage[slot_s[r], :, pl.ds(pl.multiple_of(c * 1024, 1024), 1024)]

    arrange(0, NEAR)

    def send_blocks(first, last):
        for n in range(first, last):
            remote(send.at[n], recv.at[n], ssem, rsem.at[min(n // CHUNK, CHUNKS)], here.at(ORDER[n])).start()

    q_copy.wait()
    remote(q_mine, q_all.at[row], q_ssem, q_rsem.at[0], here.at((0, 2, 0, 0))).start()
    for d in (2, 1, 3):
        remote(q_mine, q_all.at[row], q_ssem, q_rsem.at[1], here.at((d, 0, 0, 0))).start()
    send_blocks(0, NEAR)
    arrange(NEAR, DEVS)
    pl.semaphore_wait(tree.at[0], 6)
    for d in (2, 1, 3):
        pl.semaphore_signal(tree.at[1], inc=1, device_id=here.at((d, 0, 0, 0)), device_id_type=MESH)
    send_blocks(NEAR, NEAR + PLANE)
    partner = here.at((0, 2, 0, 0))[0]
    remote(q_mine, q_all.at[partner], q_ssem, q_rsem.at[0], (row, col)).wait_recv()
    for d in (2, 1, 3):
        remote(q_all.at[partner], q_all.at[partner], q_ssem, q_rsem.at[2], here.at((d, 0, 0, 0))).start()
    pl.semaphore_wait(tree.at[1], 3)
    send_blocks(NEAR + PLANE, EARLY)

    q_all[row] = q_mine[...]
    recv[DEVS - 1] = send[DEVS - 1]

    ids_copy2.wait()
    held = ids_v[...]
    mine = lax.shift_right_arithmetic(held, 7) == row
    where_to = jnp.sum(jnp.where(mine, lax.bitwise_and(held, 127), 0), axis=0, keepdims=True)
    spread = jnp.transpose(jnp.broadcast_to(where_to, (DEVS, DEVS)))
    lanes = lax.broadcasted_iota(jnp.int32, (DEVS, DEVS), 1)
    sources = lax.broadcasted_iota(jnp.int32, (DEVS, DEVS), 0)
    inverse = jnp.sum(jnp.where(spread == lanes, sources, 0), axis=0, keepdims=True)
    inv_v[...] = jnp.broadcast_to(lax.bitwise_and(inverse, 127), (8, DEVS))
    inv_copy = pltpu.make_async_copy(inv_v, inv_s, inv_sem)
    inv_copy.start()
    for n, o in enumerate(ORDER):
        from_s[here.back(o)] = n

    q7, q3 = q_all.at[pl.ds(0, ROWS - 1)], q_all.at[pl.ds(0, 3)]
    remote(q3, q3, q_ssem, q_rsem.at[1], (row, col)).wait_recv()
    remote(q3, q3, q_ssem, q_rsem.at[2], (row, col)).wait_recv()
    remote(q7, q7, q_ssem, q_rsem.at[2], (row, col)).wait_send()
    for r in range(ROWS):
        for i in range(4):
            w_rows[32 * i + 4 * r : 32 * i + 4 * r + 4, :] = q_all[r]
    w_all = jnp.transpose(w_rows[...])
    w_high = w_all.astype(jnp.bfloat16)
    w[:, 0:128] = w_high
    w[:, 128:256] = (w_all - w_high.astype(jnp.float32)).astype(jnp.bfloat16)

    def multiply(rows, to):
        high = rows.astype(jnp.bfloat16)
        low = (rows - high.astype(jnp.float32)).astype(jnp.bfloat16)
        first = jnp.dot(high, w[...], preferred_element_type=jnp.float32)
        second = jnp.dot(low, w[:, 0:128], preferred_element_type=jnp.float32)
        product = first[:, 0:128] + (first[:, 128:256] + second)
        squares = jnp.sum(rows * rows, axis=1, keepdims=True)
        for j in range(rows.shape[0] // 8):
            to(j, product[8 * j : 8 * j + 8], jnp.broadcast_to(squares[8 * j : 8 * j + 8], (8, 128)))

    lane = lax.broadcasted_iota(jnp.int32, (8, 128), 1)

    def keep_own(j, product, squares):
        own_part[j] = jnp.where(lane < 32, product, squares)

    multiply(send[BULK:DEVS].reshape(ROWS * 8, 1024), keep_own)
    own_recv[ROWS - 1] = own_part[ROWS - 1]
    for j in range(ROWS - 1):
        remote(own_part.at[j], own_recv.at[j], o_ssem, o_rsem, here.at(ORDER[BULK + j])).start()
    send_blocks(EARLY, DEVS - 1)

    inv_copy.wait()

    @pl.loop(0, DEVS, unroll=8)
    def _(p):
        here_s[p] = from_s[inv_s[0, p]]

    def arrived(i, count):
        v = recv.at[pl.ds(0, count)]
        remote(v, v, ssem, rsem.at[i], (row, col)).wait_recv()

    def product(first, count):
        def keep(j, product, squares):
            part[first + j, 0] = product
            part[first + j, 1] = squares

        multiply(recv[pl.ds(first, count)].reshape(count * 8, 1024), keep)

    @pl.loop(0, CHUNKS - 1)
    def _(i):
        arrived(i, CHUNK)
        product(i * CHUNK, CHUNK)

    o7 = own_recv.at[pl.ds(0, ROWS - 1)]
    remote(o7, o7, o_ssem, o_rsem, (row, col)).wait()
    for j in range(ROWS):
        both = own_recv[j]
        once = jnp.where(lane < 32, both, 0.0)
        twice = once + pltpu.roll(once, 32, axis=1)
        part[BULK + j, 0] = twice + pltpu.roll(twice, 64, axis=1)
        part[BULK + j, 1] = jnp.where(lane < 32, pltpu.roll(both, 64, axis=1), both)

    arrived(CHUNKS - 1, CHUNK)
    product(BULK - CHUNK, CHUNK)

    sublane = lax.broadcasted_iota(jnp.int32, (8, 128), 0)
    diagonal = (lax.rem(lane, 8) == sublane) & (lane < 64)

    def gather(c, p_to, s_to):
        for t in range(2):
            tile = part[here_s[c * 8 + t * 4], 0]
            for i in range(1, 4):
                tile = jnp.where(lane < 32 * i, tile, part[here_s[c * 8 + t * 4 + i], 0])
            p_to[t] = tile
        tile = part[here_s[c * 8], 1]
        for i in range(1, 8):
            tile = jnp.where(lane < 8 * i, tile, part[here_s[c * 8 + i], 1])
        s_to[...] = jnp.sum(jnp.where(diagonal, tile, 0.0), axis=0, keepdims=True)

    across = [(0, b, z, k) for z in range(4) for b in range(2) for k in range(2) if (b, z, k) != (0, 0, 0)]
    across = sorted(across, key=distance, reverse=True)

    def column(o):
        return here.z_col[o[2]] + here.y_col[o[1]] + here.core[o[3]]

    def share(some):
        for o in some:
            c = column(o)
            remote(p_send.at[c], p_recv.at[col], p_ssem, p_rsem, (row, c)).start()
            remote(s_send.at[c], s_recv.at[col], s_ssem, s_rsem, (row, c)).start()

    for first in range(0, 16, 4):
        for o in across[first : first + 4]:
            gather(column(o), p_send.at[column(o)], s_send.at[column(o)])
        if first:
            share(across[first - 4 : first])
    share(across[12:])
    gather(col, p_recv.at[col], s_recv.at[col])
    arrived(CHUNKS, ROWS - 1)

    @pl.loop(0, DEVS, unroll=8)
    def _(p):
        relaid[p] = recv[here_s[p]]

    p15 = p_recv.at[pl.ds(0, COLS - 1)]
    remote(p15, p15, p_ssem, p_rsem, (row, col)).wait()
    s15 = s_recv.at[pl.ds(0, COLS - 1)]
    remote(s15, s15, s_ssem, s_rsem, (row, col)).wait()
    v = recv.at[pl.ds(0, DEVS - 1)]
    remote(v, v, ssem, rsem.at[0], (row, col)).wait_send()


PIECES = 4


def finish(block, shares, squares, relaid, p_out, norm_out, p_done, norm_done, sem, small_sem):
    step = DEVS // PIECES
    copies = [
        pltpu.make_async_copy(block.at[pl.ds(i * step, step)], relaid.at[pl.ds(i * step, step)], sem.at[i])
        for i in range(PIECES)
    ]
    for copy in copies:
        copy.start()
    total, square = shares[0], squares[0]
    for c in range(1, COLS):
        total, square = total + shares[c], square + squares[c]
    norm_done[...] = jnp.sqrt(square[:, 0:64] / 16384.0 + epsilon)
    rows = []
    for g in range(8):
        t, i = divmod(g, 4)
        rows.append(total[t] if i == 0 else pltpu.roll(total[t], 128 - 32 * i, axis=1))
    p_done[...] = jnp.transpose(jnp.concatenate(rows + rows, axis=0))[0:32, 0:64]
    small = [
        pltpu.make_async_copy(norm_done, norm_out, small_sem.at[0]),
        pltpu.make_async_copy(p_done, p_out, small_sem.at[1]),
    ]
    for copy in small:
        copy.start()
    for copy in copies + small:
        copy.wait()


def on_device(old_residual, group_map, q_factor):
    f32, i32 = jnp.float32, jnp.int32
    hbm = pl.BlockSpec(memory_space=pltpu.HBM)
    vmem = pl.BlockSpec(memory_space=pltpu.VMEM)
    dma = pltpu.SemaphoreType.DMA
    given = [
        pltpu.with_memory_space_constraint(a, pltpu.HBM)
        for a in (old_residual.reshape(ROWS, 8, 16384), group_map.T, q_factor.T)
    ]
    block, shares, squares = pl.pallas_call(
        exchange,
        out_shape=(
            jax.ShapeDtypeStruct((DEVS, 8, 1024), f32),
            jax.ShapeDtypeStruct((COLS, 2, 8, 128), f32),
            jax.ShapeDtypeStruct((COLS, 1, 128), f32),
        ),
        in_specs=[hbm, hbm, hbm],
        out_specs=(vmem, vmem, vmem),
        scratch_shapes=[
            pltpu.VMEM((ROWS, 8, 16384), f32),
            pltpu.VMEM((DEVS, 8, 1024), f32),
            pltpu.VMEM((DEVS, 8, 1024), f32),
            pltpu.SMEM((8, 128), i32),
            pltpu.VMEM((8, 128), i32),
            pltpu.VMEM((4, 1024), f32),
            pltpu.VMEM((ROWS, 4, 1024), f32),
            pltpu.VMEM((128, 1024), f32),
            pltpu.VMEM((1024, 256), jnp.bfloat16),
            pltpu.VMEM((DEVS, 2, 8, 128), f32),
            pltpu.VMEM((ROWS, 8, 128), f32),
            pltpu.VMEM((ROWS, 8, 128), f32),
            pltpu.VMEM((COLS, 2, 8, 128), f32),
            pltpu.VMEM((COLS, 1, 128), f32),
            pltpu.VMEM((8, 128), i32),
            pltpu.SMEM((8, 128), i32),
            pltpu.SMEM((ROWS,), i32),
            pltpu.SMEM((DEVS,), i32),
            pltpu.SMEM((DEVS,), i32),
            dma((COLS,)),
            dma((2,)),
            dma,
            dma,
            dma,
            dma((3,)),
            dma,
            dma((CHUNKS + 1,)),
            dma,
            dma,
            dma,
            dma,
            dma,
            dma,
            pltpu.SemaphoreType.REGULAR((2,)),
        ],
        compiler_params=pltpu.CompilerParams(
            collective_id=0, has_side_effects=True, vmem_limit_bytes=40 << 20
        ),
    )(*given)
    relaid, projection, norms = pl.pallas_call(
        finish,
        out_shape=(
            jax.ShapeDtypeStruct((DEVS, 8, 1024), f32),
            jax.ShapeDtypeStruct((32, 64), f32),
            jax.ShapeDtypeStruct((1, 64), f32),
        ),
        in_specs=[vmem, vmem, vmem],
        out_specs=(hbm, hbm, hbm),
        scratch_shapes=[pltpu.VMEM((32, 64), f32), pltpu.VMEM((1, 64), f32), dma((PIECES,)), dma((2,))],
        compiler_params=pltpu.CompilerParams(vmem_limit_bytes=16 << 20),
    )(block, shares, squares)
    return relaid.reshape(1024, 1024), projection, norms.reshape(64)


def solution(mesh):
    return jax.shard_map(
        on_device,
        mesh=mesh,
        in_specs=(P(("row", "col"), None), P(), P("col", "row")),
        out_specs=(P("row", "col"), P(None, ("row", "col")), P(("row", "col"))),
        check_vma=False,
    )
```
